32 devices in a mesh: gx: 2 (over y), gy: 4 (over x, core), gz: 4 (over z).
Axes of the slice: x: 2, y: 2, z: 4, core: 2. Of those that a mesh axis runs over, the one named last changes fastest.
Arguments:
- head_out: bfloat16 [768, 4096], P(('gy', 'gx'), 'gz'), may hold values from -6 to 6
- out_weight: bfloat16 [4096, 4096], P('gz', ('gx', 'gy')), may hold values from -0.09375 to 0.09375
- residual: bfloat16 [768, 4096], P(('gy', 'gz'), 'gx'), may hold values from -84 to 84
- norm_gain: bfloat16 [4096], replicated, may hold values from 0.5 to 1.5
Outputs:
- hidden_out: bfloat16 [768, 4096], P(('gy', 'gz'), 'gx')
- normed: bfloat16 [768, 4096], P(('gy', 'gz'), 'gx')
The draws below stay inside these ranges and needn't reach their ends.
All inputs are finite; a program needn't handle non-finite values.
Results may differ from the reference program's by a relative error of at most 0.0098.
Values may be sent and summed in bfloat16 or wider, within the bound.
A program may use at most 64 MiB of HBM per device.

```python
import math
import jax
import jax.numpy as jnp
from jax import lax

D = 4096
FEATURES = 4096
TOKENS = 768


def draw_residual(key, part):
    key_base, key_rows, key_cols = jax.random.split(jax.random.fold_in(key, 11), 3)
    col_pos = jnp.arange(D, dtype=jnp.float32) / D
    col_ramp = jnp.exp((col_pos - 0.5) * math.log(3.0))
    col_spread = jnp.exp(jax.random.uniform(key_cols, (1, D), jnp.float32, math.log(0.5), math.log(2.0)))
    base_draw = jnp.clip(jax.random.normal(key_base, (TOKENS, D), jnp.float32), -6.0, 6.0)
    row_scale = jnp.exp(jax.random.uniform(key_rows, (TOKENS, 1), jnp.float32, math.log(0.4), math.log(4.0)))
    return (base_draw * row_scale * col_spread * col_ramp[None, :]).astype(jnp.bfloat16)


def with_spikes(result, key, source, target, parts, factor):
    owner, partner = [(jnp.arange(result.shape[axis_at]) // (result.shape[axis_at] // parts)).reshape([-1 if axis == axis_at else 1 for axis in range(result.ndim)]) for axis_at in (source, target)]
    chosen = jax.random.permutation(key, parts)[partner]
    strong = (owner == chosen) | (owner == (partner + parts // 2) % parts)
    return jnp.where(strong, factor * result, result)


def level_of(stream_key, extent, cuts, least, largest):
    gain = 1.0
    for position, parts in cuts:
        heights = jax.random.uniform(jax.random.fold_in(jax.random.fold_in(stream_key, 6), position), (parts,), jnp.float32, least / len(cuts), largest / len(cuts))
        gain = gain * jnp.repeat(jnp.exp(heights), extent[position] // parts).reshape((-1,) + (1,) * (len(extent) - 1 - position))
    return gain


def gaussian(key, extent, deviation, bound, shards=(), kind=jnp.bfloat16):
    values = deviation * jax.random.normal(key, extent, jnp.float32)
    if shards:
        values = values * level_of(key, extent, shards, -0.22, 0.18)
    return jnp.clip(values, -bound, bound).astype(kind)


def noise_with(own_key, shape, spread, most, shards, heavy, held_as=jnp.bfloat16):
    entries = spread * jax.random.normal(own_key, shape, jnp.float32)
    if shards:
        entries = entries * level_of(own_key, shape, shards, -0.22, 0.18)
    return jnp.clip(with_spikes(entries, jax.random.fold_in(own_key, 3), *heavy), -most, most).astype(held_as)


def setup_inputs(seed: int = 0) -> dict:
    key_list = jax.random.split(jax.random.key(seed), 5)
    head_out = noise_with(key_list[0], (TOKENS, FEATURES), 1.0, 6.0, ((0, 8), (1, 4)), (1, 0, 8, 2.0))
    out_weight = gaussian(key_list[1], (FEATURES, D), FEATURES ** -0.5, 0.09375, ((0, 4), (1, 8)))
    residual = draw_residual(jax.random.fold_in(key_list[4], 71), 0)
    norm_gain = jnp.clip(1.0 + 0.1 * jax.random.normal(key_list[3], (D,), jnp.float32), 0.5, 1.5).astype(jnp.bfloat16)
    return dict(head_out=head_out, out_weight=out_weight, residual=residual, norm_gain=norm_gain)


def reference(head_out, out_weight, residual, norm_gain):
    projected = jnp.dot(head_out, out_weight, preferred_element_type=jnp.float32)
    hidden = (residual.astype(jnp.float32) + projected).astype(jnp.bfloat16)
    widened = lax.optimization_barrier(hidden).astype(jnp.float32)
    inverse = lax.rsqrt(lax.optimization_barrier(jnp.mean(widened * widened, axis=1, keepdims=True)) + 1e-05)
    normed = (widened * inverse * norm_gain.astype(jnp.float32)).astype(jnp.bfloat16)
    return (hidden, normed)
```

```python
import functools

import jax
import jax.numpy as jnp
from jax import lax
from jax.experimental import pallas as pl
from jax.experimental.pallas import tpu as pltpu
from jax.sharding import PartitionSpec as P

MESH = pl.DeviceIdType.MESH
F32 = jnp.float32
BF16 = jnp.bfloat16
CORES = 2
W_CUTS = 4


def project(nx, ny, nz, head_ref, w_ref, res_ref, hid_ref, inv_ref,
            heads, w_own, w_other, res_v, send_buf, recv, inb, hold, own, sums,
            head_sem, w_sem, res_sem, w_send, w_recv, hx_send, hy_send, fx_send, fy_send, h_recv,
            p_send, p_recv, c_recv, s_send, s_recv):
    y = lax.axis_index("gx")
    gy = lax.axis_index("gy")
    z = lax.axis_index("gz")
    x, core = lax.div(gy, CORES), lax.rem(gy, CORES)
    out_rows, cols = res_ref.shape
    depth, wc = w_ref.shape
    half = nz // 2
    early = (half + 1) // 2
    s = lax.div(z, half)
    u = z + s * (nz - 1 - 2 * z)
    ahead = 1 - 2 * s
    last = half - 1

    def place(dx, dy, zz):
        return (lax.rem(y + dy, ny), lax.rem(x + dx + nx, nx) * CORES + core, zz)

    def target(kind, k):
        if kind == "F":
            return (1 - s) * (nz - 1) + (2 * s - 1) * k
        return s * half + lax.rem(z - s * half + k, half)

    partner = (y, x * CORES + 1 - core, z)
    border = s * half + (1 - s) * last
    facing = (1 - s) * half + s * last
    pl_sig = functools.partial(pl.semaphore_signal, inc=1, device_id_type=MESH)
    barrier = pltpu.get_barrier_semaphore()
    pl_sig(barrier, device_id=partner)
    pl_sig(barrier, device_id=place(0, 1, z))
    for dx in range(nx):
        for k in range(half):
            if (dx, k) != (0, 0):
                pl_sig(barrier, device_id=place(dx, 0, target("N", k)))
        pl_sig(barrier, device_id=place(dx, 0, facing))

    blocks = [(0, 0)]
    head_in = [pltpu.make_async_copy(head_ref.at[pl.ds(j * out_rows, out_rows)], heads.at[0, y * half + j], head_sem.at[j])
               for j in range(half)]
    step = depth // W_CUTS
    w_in = [pltpu.make_async_copy(w_ref.at[pl.ds(j * step, step)], w_own.at[pl.ds(j * step, step)], w_sem.at[j])
            for j in range(W_CUTS)]
    res_in = pltpu.make_async_copy(res_ref, res_v, res_sem)
    for copy in (*head_in, *w_in, res_in):
        copy.start()
    w_out = [pltpu.make_async_remote_copy(
        src_ref=w_own.at[pl.ds(j * step, step)], dst_ref=w_other.at[pl.ds(j * step, step)],
        send_sem=w_send.at[j], recv_sem=w_recv.at[j], device_id=partner, device_id_type=MESH) for j in range(W_CUTS)]
    for copy in head_in:
        copy.wait()
    met = 2 + nx * half - 1
    pl.semaphore_wait(barrier, met + jnp.where(u == last, nx * half, 0))

    def head_x(dx, t):
        return pltpu.make_async_remote_copy(
            src_ref=heads.at[0, t], dst_ref=heads.at[dx, t], send_sem=hx_send.at[dx, t], recv_sem=h_recv.at[dx, t],
            device_id=place(-dx, 0, z), device_id_type=MESH)

    def head_y(t):
        return pltpu.make_async_remote_copy(
            src_ref=heads.at[0, t], dst_ref=heads.at[0, t], send_sem=hy_send.at[t], recv_sem=h_recv.at[0, t],
            device_id=place(0, 1, z), device_id_type=MESH)

    def onward_y(dx, t):
        return pltpu.make_async_remote_copy(
            src_ref=heads.at[dx, t], dst_ref=heads.at[dx, t], send_sem=fy_send.at[dx, t], recv_sem=h_recv.at[dx, t],
            device_id=place(0, 1, z), device_id_type=MESH)

    def onward_x(dx, t):
        return pltpu.make_async_remote_copy(
            src_ref=heads.at[0, t], dst_ref=heads.at[dx, t], send_sem=fx_send.at[dx, t], recv_sem=h_recv.at[dx, t],
            device_id=place(-dx, 0, z), device_id_type=MESH)

    def landed(dx, t):
        head_x(dx, t).wait_recv()

    def slot(kind, k):
        return k if kind == "F" else half + k

    def to_owner(dx, kind, k, hr):
        n = slot(kind, k)
        return pltpu.make_async_remote_copy(
            src_ref=send_buf.at[dx, n, hr], dst_ref=recv.at[dx, half if kind == "F" else k, hr],
            send_sem=p_send.at[dx, n, hr], recv_sem=p_recv.at[dx, half if kind == "F" else k, hr],
            device_id=place(dx, 0, target(kind, k)), device_id_type=MESH)

    def to_next(dx, k, hr):
        return pltpu.make_async_remote_copy(
            src_ref=send_buf.at[dx, k, hr], dst_ref=inb.at[dx, k, hr],
            send_sem=p_send.at[dx, k, hr], recv_sem=c_recv.at[dx, k, hr],
            device_id=place(0, 0, z + ahead), device_id_type=MESH)

    def compute(dx, kind, k, hr):
        part = jnp.dot(heads[dx, target(kind, k)], (w_other if hr else w_own)[...], preferred_element_type=F32)
        if kind == "N":
            if (dx, k) == (0, 0):
                own[hr] = part
            else:
                send_buf[dx, slot(kind, k), hr] = part.astype(BF16)
                to_owner(dx, kind, k, hr).start()
        else:
            @pl.when(u == 0)
            def _():
                send_buf[dx, k, hr] = part.astype(BF16)
                to_next(dx, k, hr).start()

            @pl.when(u > 0)
            def _():
                hold[dx, k, hr] = part

    def both(dx, kind, k):
        for hr in range(CORES):
            compute(dx, kind, k, hr)

    def merge(dx, k):
        @pl.when(u > 0)
        def _():
            for hr in range(CORES):
                to_next(dx, k, hr).wait_recv()
                send_buf[dx, k, hr] = (hold[dx, k, hr] + inb[dx, k, hr].astype(F32)).astype(BF16)
                if half > 2:
                    pl.when(u < last)(to_next(dx, k, hr).start)
                pl.when(u == last)(to_owner(dx, "F", k, hr).start)

    near = [(k + 1) % half for k in range(half)]
    far = list(range(half))
    others = range(1, nx)

    def run(mine, theirs, merges):
        (mk, mo), (tk, to) = mine, theirs
        for k in mo:
            t = target(mk, k)
            head_y(t).start()
            for dx in others:
                head_x(dx, t).start()
        for j in range(W_CUTS):
            w_in[j].wait()
            w_out[j].start()
        for k in mo:
            compute(0, mk, k, 0)
        for copy in w_out:
            copy.wait_recv()
        for k in mo:
            compute(0, mk, k, 1)
        for o in range(half):
            def x_side(o=o):
                for dx in others:
                    t = target(mk, mo[o])
                    landed(dx, t)
                    if o < early:
                        onward_y(dx, t).start()
                    both(dx, mk, mo[o])

            def y_side(o=o):
                t = target(tk, to[o])
                landed(0, t)
                if o >= early:
                    for dx in others:
                        onward_x(dx, t).start()
                both(0, tk, to[o])

            if mk == "N":
                y_side()
                x_side()
            else:
                x_side()
                y_side()
        if mk == "F":
            for k in mo:
                merge(0, k)
        for o in range(half):
            for dx in others:
                landed(dx, target(tk, to[o]))
                both(dx, tk, to[o])
        for dx in range(1 if mk == "F" else 0, nx):
            for k in far:
                merge(dx, k)
        for o in range(half):
            t = target(mk, mo[o])
            head_y(t).wait_send()
            for dx in others:
                head_x(dx, t).wait_send()
                if o < early:
                    onward_y(dx, t).wait_send()
                else:
                    onward_x(dx, target(tk, to[o])).wait_send()

    pl.when(y == s)(lambda: run(("N", near), ("F", far), 0))
    pl.when(y != s)(lambda: run(("F", far), ("N", near), 0))

    res_in.wait()
    total = jnp.zeros((out_rows, 128), F32)
    for dx in range(nx):
        from_x = lax.rem(x - dx + nx, nx)
        for hr in range(CORES):
            side = core if hr == 0 else 1 - core
            where = pl.ds(pl.multiple_of((from_x * CORES + side) * wc, wc), wc)
            acc = own[hr] if dx == 0 else None
            for k in range(half + 1):
                if (dx, k) == (0, 0):
                    continue
                pltpu.make_async_remote_copy(
                    src_ref=send_buf.at[0, 0, hr], dst_ref=recv.at[dx, k, hr],
                    send_sem=p_send.at[0, 0, hr], recv_sem=p_recv.at[dx, k, hr],
                    device_id=partner, device_id_type=MESH).wait_recv()
                term = recv[dx, k, hr].astype(F32)
                acc = term if acc is None else acc + term
            hidden = (res_v[:, where].astype(F32) + acc).astype(BF16)
            hid_ref[:, where] = hidden
            wide = hidden.astype(F32)
            square = wide * wide
            for k in range(0, wc, 128):
                total = total + square[:, k:k + 128]
    sums[0] = jnp.broadcast_to(jnp.sum(total, axis=1, keepdims=True), (out_rows, 128))
    swap = pltpu.make_async_remote_copy(
        src_ref=sums.at[0], dst_ref=sums.at[1], send_sem=s_send, recv_sem=s_recv,
        device_id=place(0, 1, z), device_id_type=MESH)
    swap.start()

    for copy in w_out:
        copy.wait_send()
    for dx in range(nx):
        for hr in range(CORES):
            for k in range(half):
                if (dx, k) != (0, 0):
                    to_owner(dx, "N", k, hr).wait_send()
                to_next(dx, k, hr).wait_send()
    swap.wait()
    inv_ref[...] = lax.rsqrt((sums[0] + sums[1]) / (cols * ny) + 1e-05)


def finish(hid_ref, inv_ref, gain_ref, out_hid, out_nrm, nrm, sems):
    y = lax.axis_index("gx")
    cols = hid_ref.shape[1]
    first = pltpu.make_async_copy(hid_ref, out_hid, sems.at[0])
    first.start()
    gain = gain_ref[pl.ds(pl.multiple_of(y * cols, cols), cols)].astype(F32).reshape(1, cols)
    nrm[...] = (hid_ref[...].astype(F32) * inv_ref[:, :1] * gain).astype(BF16)
    second = pltpu.make_async_copy(nrm, out_nrm, sems.at[1])
    second.start()
    first.wait()
    second.wait()


def shards(head_out, out_weight, residual, norm_gain):
    ny, ngy, nz = (lax.axis_size(a) for a in ("gx", "gy", "gz"))
    nx = ngy // CORES
    depth, wc = out_weight.shape
    out_rows, cols = residual.shape
    half = nz // 2
    if ny != 2 or nz % 2 or half < 2:
        raise ValueError("unsupported mesh")
    any_spec = pl.BlockSpec(memory_space=pl.ANY)
    vmem = pl.BlockSpec(memory_space=pltpu.VMEM)
    dma = pltpu.SemaphoreType.DMA
    hidden, inverse = pl.pallas_call(
        functools.partial(project, nx, ny, nz),
        out_shape=[pltpu.VMEM((out_rows, cols), BF16), pltpu.VMEM((out_rows, 128), F32)],
        in_specs=[any_spec] * 3,
        out_specs=[vmem, vmem],
        scratch_shapes=[
            pltpu.VMEM((nx, nz, out_rows, depth), BF16),
            pltpu.VMEM((depth, wc), BF16),
            pltpu.VMEM((depth, wc), BF16),
            pltpu.VMEM((out_rows, cols), BF16),
            pltpu.VMEM((nx, nz, CORES, out_rows, wc), BF16),
            pltpu.VMEM((nx, half + 1, CORES, out_rows, wc), BF16),
            pltpu.VMEM((nx, half, CORES, out_rows, wc), BF16),
            pltpu.VMEM((nx, half, CORES, out_rows, wc), F32),
            pltpu.VMEM((CORES, out_rows, wc), F32),
            pltpu.VMEM((ny, out_rows, 128), F32),
            dma((half,)), dma((W_CUTS,)), dma, dma((W_CUTS,)), dma((W_CUTS,)),
            dma((nx, nz)), dma((nz,)), dma((nx, nz)), dma((nx, nz)), dma((nx, nz)),
            dma((nx, nz, CORES)), dma((nx, half + 1, CORES)), dma((nx, half, CORES)),
            dma, dma,
        ],
        compiler_params=pltpu.CompilerParams(collective_id=0, has_side_effects=True),
    )(head_out, out_weight, residual)
    return pl.pallas_call(
        finish,
        out_shape=[jax.ShapeDtypeStruct((out_rows, cols), BF16)] * 2,
        in_specs=[vmem] * 3,
        out_specs=[any_spec] * 2,
        scratch_shapes=[pltpu.VMEM((out_rows, cols), BF16), dma((2,))],
    )(*(pltpu.with_memory_space_constraint(a, pltpu.VMEM) for a in (hidden, inverse)), norm_gain)


def solution(mesh):
    in_specs = (P(("gy", "gx"), "gz"), P("gz", ("gx", "gy")), P(("gy", "gz"), "gx"), P())
    out_specs = (P(("gy", "gz"), "gx"), P(("gy", "gz"), "gx"))
    return jax.shard_map(shards, mesh=mesh, in_specs=in_specs, out_specs=out_specs, check_vma=False)
```

```python
import functools

import jax
import jax.numpy as jnp
from jax import lax
from jax.experimental import pallas as pl
from jax.experimental.pallas import tpu as pltpu
from jax.sharding import PartitionSpec as P

MESH = pl.DeviceIdType.MESH
F32 = jnp.float32
BF16 = jnp.bfloat16
CORES = 2
W_CUTS = 4
FINISH_CUTS = 3


def project(nx, ny, nz, head_ref, w_ref, res_ref, gain_ref, hid_ref, inv_ref, gain_out,
            heads, w_own, w_other, res_v, gain_v, send_buf, recv, inb, hold, own, sums,
            in_sem, w_sem, w_send, w_recv, h_send, h_recv, p_send, n_recv, m_recv, c_recv, s_send, s_recv, up_sem, down_sem):
    y = lax.axis_index("gx")
    gy = lax.axis_index("gy")
    z = lax.axis_index("gz")
    x, core = lax.div(gy, CORES), lax.rem(gy, CORES)
    out_rows, cols = res_ref.shape
    depth, wc = w_ref.shape
    half = nz // 2
    early = (half + 1) // 2
    s = lax.div(z, half)
    u = z + s * (nz - 1 - 2 * z)
    ahead = 1 - 2 * s
    last = half - 1

    def place(dx, dy, zz):
        return (lax.rem(y + dy, ny), lax.rem(x + dx + nx, nx) * CORES + core, zz)

    def target(kind, k):
        if kind == "F":
            return (1 - s) * (nz - 1) + (2 * s - 1) * k
        return s * half + lax.rem(z - s * half + k, half)

    partner = (y, x * CORES + 1 - core, z)
    pl_sig = functools.partial(pl.semaphore_signal, inc=1, device_id_type=MESH)
    barrier = pltpu.get_barrier_semaphore()
    pl_sig(barrier, device_id=partner)
    pl_sig(barrier, device_id=place(0, 1, z))
    for dx in range(1, nx):
        pl_sig(barrier, device_id=place(dx, 0, z))
    below, above = z > 0, z < nz - 1
    pl.when(below)(lambda: pl_sig(barrier, device_id=place(0, 0, z - 1)))
    pl.when(above)(lambda: pl_sig(barrier, device_id=place(0, 0, z + 1)))

    mine = heads.at[pl.ds(y * half, half)]
    head_in = pltpu.make_async_copy(head_ref, mine, in_sem.at[0])
    step = depth // W_CUTS
    w_in = [pltpu.make_async_copy(w_ref.at[pl.ds(j * step, step)], w_own.at[pl.ds(j * step, step)], w_sem.at[j])
            for j in range(W_CUTS)]
    res_in = pltpu.make_async_copy(res_ref, res_v, in_sem.at[1])
    gain_in = pltpu.make_async_copy(gain_ref.at[pl.ds(pl.multiple_of(y * cols, cols), cols)], gain_v, in_sem.at[2])
    for copy in (head_in, *w_in, res_in, gain_in):
        copy.start()
    w_out = [pltpu.make_async_remote_copy(
        src_ref=w_own.at[pl.ds(j * step, step)], dst_ref=w_other.at[pl.ds(j * step, step)],
        send_sem=w_send, recv_sem=w_recv, device_id=partner, device_id_type=MESH) for j in range(W_CUTS)]
    head_in.wait()
    pl.semaphore_wait(barrier, nx + 1 + jnp.minimum(z, 1) + jnp.minimum(nz - 1 - z, 1))

    def pass_up():
        pl.when(below)(lambda: pl.semaphore_wait(up_sem, 1))
        pl.when(above)(lambda: pl_sig(up_sem, device_id=place(0, 0, z + 1)))

    def pass_down():
        pl.when(above)(lambda: pl.semaphore_wait(down_sem, 1))
        pl.when(below)(lambda: pl_sig(down_sem, device_id=place(0, 0, z - 1)))

    def meet_first():
        pl.when(s == 0)(pass_up)
        pl.when(s == 1)(pass_down)

    def meet_last():
        pl.when(s == 0)(pass_down)
        pl.when(s == 1)(pass_up)

    all_w = pltpu.make_async_remote_copy(
        src_ref=w_own, dst_ref=w_other, send_sem=w_send, recv_sem=w_recv, device_id=partner, device_id_type=MESH)

    def hop(source, dest, t, to):
        return pltpu.make_async_remote_copy(
            src_ref=heads.at[source * nz + t], dst_ref=heads.at[dest * nz + t], send_sem=h_send,
            recv_sem=h_recv.at[dest, t], device_id=to, device_id_type=MESH)

    def head_x(dx, t):
        return hop(0, dx, t, place(-dx, 0, z))

    def head_y(t):
        return hop(0, 0, t, place(0, 1, z))

    def onward_y(dx, t):
        return hop(dx, dx, t, place(0, 1, z))

    onward_x = head_x

    def landed(dx, t):
        head_x(dx, t).wait_recv()

    def slot(dx, kind, k):
        return dx * nz + (half + k if kind == "F" else k) - 1

    def arrival(dx, kind, k, hr):
        return m_recv.at[dx, hr] if kind == "F" else n_recv.at[dx]

    def to_owner(dx, kind, k, hr):
        return pltpu.make_async_remote_copy(
            src_ref=send_buf.at[slot(dx, kind, k), hr], dst_ref=recv.at[dx, half if kind == "F" else k, hr],
            send_sem=p_send, recv_sem=arrival(dx, kind, k, hr), device_id=place(dx, 0, target(kind, k)), device_id_type=MESH)

    def to_next(dx, k, hr):
        return pltpu.make_async_remote_copy(
            src_ref=send_buf.at[slot(dx, "F", k), hr], dst_ref=inb.at[dx, k, hr],
            send_sem=p_send, recv_sem=c_recv.at[dx, k, hr], device_id=place(0, 0, z + ahead), device_id_type=MESH)

    def compute(dx, kind, k, hr, send=True):
        part = jnp.dot(heads[dx * nz + target(kind, k)], (w_other if hr else w_own)[...], preferred_element_type=F32)
        if kind == "N":
            if (dx, k) == (0, 0):
                own[hr] = part
            else:
                send_buf[slot(dx, kind, k), hr] = part.astype(BF16)
                if send:
                    to_owner(dx, kind, k, hr).start()
                else:
                    pl.when(u > 0)(to_owner(dx, kind, k, hr).start)
        else:
            @pl.when(u == 0)
            def _():
                send_buf[slot(dx, "F", k), hr] = part.astype(BF16)
                to_next(dx, k, hr).start()

            @pl.when(u > 0)
            def _():
                hold[dx, k, hr] = part

    def both(dx, kind, k, send=True):
        for hr in range(CORES):
            compute(dx, kind, k, hr, send)

    def late(dx, k):
        for hr in range(CORES):
            pl.when(u == 0)(to_owner(dx, "N", k, hr).start)

    def merge(dx, k):
        @pl.when(u > 0)
        def _():
            for hr in range(CORES):
                to_next(dx, k, hr).wait_recv()
                send_buf[slot(dx, "F", k), hr] = (hold[dx, k, hr] + inb[dx, k, hr].astype(F32)).astype(BF16)
                if half > 2:
                    pl.when(u < last)(to_next(dx, k, hr).start)
                pl.when(u == last)(to_owner(dx, "F", k, hr).start)

    near = far = list(range(half))
    others = range(1, nx)

    def run(local, distant):
        (mk, mo), (tk, to) = local, distant

        def x_out(o):
            for dx in others:
                head_x(dx, target(mk, mo[o])).start()

        for o in range(half):
            head_y(target(mk, mo[o])).start()
            r = half - 1 - o
            if mk == "F" or r >= early:
                x_out(r)
        for j in range(W_CUTS):
            w_in[j].wait()
            w_out[j].start()
        meet_first()
        if half > 2:
            meet_last()
        for k in reversed(mo) if mk == "N" else mo:
            compute(0, mk, k, 0)
        all_w.wait_recv()
        for k in reversed(mo) if mk == "N" else mo:
            compute(0, mk, k, 1)

        def x_land(o):
            for dx in others:
                t = target(mk, mo[o])
                landed(dx, t)
                if o >= early:
                    onward_y(dx, t).start()

        def y_land(o):
            t = target(tk, to[o])
            landed(0, t)
            if o < early:
                for dx in others:
                    onward_x(dx, t).start()

        def diagonal(o):
            for dx in others:
                landed(dx, target(tk, to[o]))
                both(dx, tk, to[o])

        if mk == "N":
            for o in range(half):
                y_land(o)
                if o < early:
                    x_out(early - 1 - o)
                both(0, tk, to[o])
                if half - 1 - o >= early:
                    x_land(half - 1 - o)
        else:
            for o in range(half):
                x_land(half - 1 - o)
                for dx in others:
                    both(dx, mk, mo[half - 1 - o])
                y_land(o)
        if half == 2:
            meet_last()
        if mk == "N":
            for r in reversed(range(early, half)):
                for dx in others:
                    both(dx, mk, mo[r], send=False)
            merge(0, far[0])
            for o in range(half):
                diagonal(o)
            for k in far[1:]:
                merge(0, k)
            for r in reversed(range(early)):
                x_land(r)
                for dx in others:
                    both(dx, mk, mo[r], send=mo[r] == 0)
            for k in far:
                for dx in others:
                    merge(dx, k)
            for k in range(1, half):
                for dx in others:
                    late(dx, k)
        else:
            for k in far:
                merge(0, k)
                both(0, tk, to[half - 1 - k])
            for o in reversed(range(half)):
                diagonal(o)
            for k in reversed(far):
                for dx in others:
                    merge(dx, k)

    pl.when(y == s)(lambda: run(("N", near), ("F", far)))
    pl.when(y != s)(lambda: run(("F", far), ("N", near)))

    gain_in.wait()
    gain_out[...] = gain_v[...].astype(F32).reshape(1, cols)
    res_in.wait()
    total = jnp.zeros((out_rows, 128), F32)
    for dx in range(nx):
        from_x = lax.rem(x - dx + nx, nx)
        for hr in range(CORES):
            side = core if hr == 0 else 1 - core
            where = pl.ds(pl.multiple_of((from_x * CORES + side) * wc, wc), wc)
            if hr == 0:
                group = recv.at[dx, pl.ds(1 if dx == 0 else 0, half - 1 if dx == 0 else half)]
                pltpu.make_async_remote_copy(
                    src_ref=group, dst_ref=group, send_sem=p_send, recv_sem=n_recv.at[dx],
                    device_id=partner, device_id_type=MESH).wait_recv()
            acc = own[hr] if dx == 0 else recv[dx, 0, hr].astype(F32)
            for k in range(1, half):
                acc = acc + recv[dx, k, hr].astype(F32)
            to_owner(dx, "F", 0, hr).wait_recv()
            acc = acc + recv[dx, half, hr].astype(F32)
            hidden = (res_v[:, where].astype(F32) + acc).astype(BF16)
            hid_ref[:, where] = hidden
            wide = hidden.astype(F32)
            square = wide * wide
            for k in range(0, wc, 128):
                total = total + square[:, k:k + 128]
    sums[0] = jnp.broadcast_to(jnp.sum(total, axis=1, keepdims=True), (out_rows, 128))
    swap = pltpu.make_async_remote_copy(
        src_ref=sums.at[0], dst_ref=sums.at[1], send_sem=s_send, recv_sem=s_recv,
        device_id=place(0, 1, z), device_id_type=MESH)
    swap.start()

    all_w.wait_send()
    sent = heads.at[pl.ds(0, nx * nz - half)]
    for buf, sem in ((sent, h_send), (send_buf, p_send)):
        pltpu.make_async_remote_copy(
            src_ref=buf, dst_ref=buf, send_sem=sem, recv_sem=w_recv, device_id=partner, device_id_type=MESH).wait_send()
    swap.wait()
    inv_ref[...] = lax.rsqrt((sums[0] + sums[1]) / (cols * ny) + 1e-05)


def finish(hid_ref, inv_ref, gain_ref, out_hid, out_nrm, nrm, sems):
    rows, cols = hid_ref.shape
    cut = rows // FINISH_CUTS
    whole = pltpu.make_async_copy(hid_ref, out_hid, sems.at[FINISH_CUTS])
    whole.start()
    parts = []
    for j in range(FINISH_CUTS):
        at = pl.ds(j * cut, cut)
        nrm[at] = (hid_ref[at].astype(F32) * inv_ref[at, :1] * gain_ref[...]).astype(BF16)
        parts.append(pltpu.make_async_copy(nrm.at[at], out_nrm.at[at], sems.at[j]))
        parts[-1].start()
    for copy in (whole, *parts):
        copy.wait()


def shards(head_out, out_weight, residual, norm_gain):
    ny, ngy, nz = (lax.axis_size(a) for a in ("gx", "gy", "gz"))
    nx = ngy // CORES
    depth, wc = out_weight.shape
    out_rows, cols = residual.shape
    half = nz // 2
    if ny != 2 or nz % 2 or half < 2:
        raise ValueError("unsupported mesh")
    any_spec = pl.BlockSpec(memory_space=pl.ANY)
    vmem = pl.BlockSpec(memory_space=pltpu.VMEM)
    dma, regular = pltpu.SemaphoreType.DMA, pltpu.SemaphoreType.REGULAR
    held = pl.pallas_call(
        functools.partial(project, nx, ny, nz),
        out_shape=[pltpu.VMEM((out_rows, cols), BF16), pltpu.VMEM((out_rows, 128), F32), pltpu.VMEM((1, cols), F32)],
        in_specs=[any_spec] * 4,
        out_specs=[vmem] * 3,
        scratch_shapes=[
            pltpu.VMEM((nx * nz, out_rows, depth), BF16),
            pltpu.VMEM((depth, wc), BF16),
            pltpu.VMEM((depth, wc), BF16),
            pltpu.VMEM((out_rows, cols), BF16),
            pltpu.VMEM((cols,), BF16),
            pltpu.VMEM((nx * nz - 1, CORES, out_rows, wc), BF16),
            pltpu.VMEM((nx, half + 1, CORES, out_rows, wc), BF16),
            pltpu.VMEM((nx, half, CORES, out_rows, wc), BF16),
            pltpu.VMEM((nx, half, CORES, out_rows, wc), F32),
            pltpu.VMEM((CORES, out_rows, wc), F32),
            pltpu.VMEM((ny, out_rows, 128), F32),
            dma((3,)), dma((W_CUTS,)), dma, dma, dma, dma((nx, nz)),
            dma, dma((nx,)), dma((nx, CORES)), dma((nx, half, CORES)), dma, dma, regular, regular,
        ],
        compiler_params=pltpu.CompilerParams(collective_id=0, has_side_effects=True),
    )(head_out.reshape(half, out_rows, depth), out_weight, residual, norm_gain)
    return pl.pallas_call(
        finish,
        out_shape=[jax.ShapeDtypeStruct((out_rows, cols), BF16)] * 2,
        in_specs=[vmem] * 3,
        out_specs=[any_spec] * 2,
        scratch_shapes=[pltpu.VMEM((out_rows, cols), BF16), dma((FINISH_CUTS + 1,))],
    )(*(pltpu.with_memory_space_constraint(a, pltpu.VMEM) for a in held))


def solution(mesh):
    in_specs = (P(("gy", "gx"), "gz"), P("gz", ("gx", "gy")), P(("gy", "gz"), "gx"), P())
    out_specs = (P(("gy", "gz"), "gx"), P(("gy", "gz"), "gx"))
    return jax.shard_map(shards, mesh=mesh, in_specs=in_specs, out_specs=out_specs, check_vma=False)
```

```python
import functools

import jax
import jax.numpy as jnp
from jax import lax
from jax.experimental import pallas as pl
from jax.experimental.pallas import tpu as pltpu
from jax.sharding import PartitionSpec as P

MESH = pl.DeviceIdType.MESH
F32 = jnp.float32
BF16 = jnp.bfloat16
CORES = 2
W_CUTS = 4
FINISH_CUTS = 3


def project(nx, ny, nz, head_ref, w_ref, res_ref, gain_ref, hid_ref, inv_ref, gain_out,
            mine, heads, w_own, w_other, res_v, gain_v, send_buf, recv, inb, hold, sums,
            in_sem, w_sem, w_send, w_recv, h_send, h_recv, p_send, n_recv, m_recv, c_recv, s_send, s_recv, up_sem, down_sem):
    y = lax.axis_index("gx")
    gy = lax.axis_index("gy")
    z = lax.axis_index("gz")
    x, core = lax.div(gy, CORES), lax.rem(gy, CORES)
    out_rows, cols = res_ref.shape
    depth, wc = w_ref.shape
    half = nz // 2
    early = (half + 1) // 2
    s = lax.div(z, half)
    u = z + s * (nz - 1 - 2 * z)
    ahead = 1 - 2 * s
    last = half - 1

    def place(dx, dy, zz, side=core):
        return (lax.rem(y + dy, ny), lax.rem(x + dx + nx, nx) * CORES + side, zz)

    def target(kind, k):
        if kind == "F":
            return (1 - s) * (nz - 1) + (2 * s - 1) * k
        return s * half + lax.rem(z - s * half + k, half)

    cross = 1 - core
    partner = place(0, 0, z, cross)
    pl_sig = functools.partial(pl.semaphore_signal, inc=1, device_id_type=MESH)
    barrier = pltpu.get_barrier_semaphore()
    pl_sig(barrier, device_id=partner)
    below, above = z > 0, z < nz - 1
    for side in (core, cross):
        pl_sig(barrier, device_id=place(0, 1, z, side))
        for dx in range(1, nx):
            pl_sig(barrier, device_id=place(dx, 0, z, side))
        pl.when(below)(lambda: pl_sig(barrier, device_id=place(0, 0, z - 1, side)))
        pl.when(above)(lambda: pl_sig(barrier, device_id=place(0, 0, z + 1, side)))

    head_in = pltpu.make_async_copy(head_ref, mine, in_sem.at[0])
    step = depth // W_CUTS
    w_in = [pltpu.make_async_copy(w_ref.at[pl.ds(j * step, step)], w_own.at[pl.ds(j * step, step)], w_sem.at[j])
            for j in range(W_CUTS)]
    res_in = pltpu.make_async_copy(res_ref, res_v, in_sem.at[1])
    gain_in = pltpu.make_async_copy(gain_ref.at[pl.ds(pl.multiple_of(y * cols, cols), cols)], gain_v, in_sem.at[2])
    for copy in (head_in, *w_in, res_in, gain_in):
        copy.start()
    w_out = [pltpu.make_async_remote_copy(
        src_ref=w_own.at[pl.ds(j * step, step)], dst_ref=w_other.at[pl.ds(j * step, step)],
        send_sem=w_send, recv_sem=w_recv, device_id=partner, device_id_type=MESH) for j in range(W_CUTS)]
    head_in.wait()
    pl.semaphore_wait(barrier, 1 + CORES * (nx + jnp.minimum(z, 1) + jnp.minimum(nz - 1 - z, 1)))

    def pass_up():
        pl.when(below)(lambda: pl.semaphore_wait(up_sem, 1))
        pl.when(above)(lambda: pl_sig(up_sem, device_id=place(0, 0, z + 1)))

    def pass_down():
        pl.when(above)(lambda: pl.semaphore_wait(down_sem, 1))
        pl.when(below)(lambda: pl_sig(down_sem, device_id=place(0, 0, z - 1)))

    def meet_first():
        pl.when(s == 0)(pass_up)
        pl.when(s == 1)(pass_down)

    def meet_last():
        pl.when(s == 0)(pass_down)
        pl.when(s == 1)(pass_up)

    all_w = pltpu.make_async_remote_copy(
        src_ref=w_own, dst_ref=w_other, send_sem=w_send, recv_sem=w_recv, device_id=partner, device_id_type=MESH)

    def hop(source, dx, t, to):
        return pltpu.make_async_remote_copy(
            src_ref=source, dst_ref=heads.at[dx * nz + t], send_sem=h_send,
            recv_sem=h_recv.at[dx, t], device_id=to, device_id_type=MESH)

    def head_out(dx, dy, t):
        return hop(mine.at[t - y * half], dx, t, place(-dx, dy, z, cross))

    def onward_y(dx, t):
        return hop(heads.at[dx * nz + t], dx, t, place(0, 1, z))

    def onward_x(dx, t):
        return hop(heads.at[t], dx, t, place(-dx, 0, z))

    def landed(dx, t):
        onward_y(dx, t).wait_recv()

    def slot(dx, kind, k):
        return dx * nz + (half + k if kind == "F" else k)

    def arrival(dx, kind, k, hr):
        return m_recv.at[dx, hr] if kind == "F" else n_recv.at[dx]

    def to_owner(dx, kind, k, hr):
        return pltpu.make_async_remote_copy(
            src_ref=send_buf.at[slot(dx, kind, k), hr], dst_ref=recv.at[dx, half if kind == "F" else k, hr],
            send_sem=p_send, recv_sem=arrival(dx, kind, k, hr), device_id=place(dx, 0, target(kind, k), cross), device_id_type=MESH)

    def to_next(dx, k, hr):
        return pltpu.make_async_remote_copy(
            src_ref=send_buf.at[slot(dx, "F", k), hr], dst_ref=inb.at[dx, k, hr],
            send_sem=p_send, recv_sem=c_recv.at[dx, k, hr], device_id=place(0, 0, z + ahead), device_id_type=MESH)

    def compute(dx, kind, k, hr, send=True):
        part = jnp.dot(heads[dx * nz + target(kind, k)], (w_other if hr else w_own)[...], preferred_element_type=F32)
        if kind == "N":
            send_buf[slot(dx, kind, k), hr] = part.astype(BF16)
            if send:
                to_owner(dx, kind, k, hr).start()
            else:
                pl.when(u > 0)(to_owner(dx, kind, k, hr).start)
        else:
            @pl.when(u == 0)
            def _():
                send_buf[slot(dx, "F", k), hr] = part.astype(BF16)
                to_next(dx, k, hr).start()

            @pl.when(u > 0)
            def _():
                hold[dx, k, hr] = part

    def both(dx, kind, k, send=True):
        for hr in range(CORES):
            compute(dx, kind, k, hr, send)

    def late(dx, k):
        for hr in range(CORES):
            pl.when(u == 0)(to_owner(dx, "N", k, hr).start)

    def merge(dx, k):
        @pl.when(u > 0)
        def _():
            for hr in range(CORES):
                to_next(dx, k, hr).wait_recv()
                send_buf[slot(dx, "F", k), hr] = (hold[dx, k, hr] + inb[dx, k, hr].astype(F32)).astype(BF16)
                if half > 2:
                    pl.when(u < last)(to_next(dx, k, hr).start)
                pl.when(u == last)(to_owner(dx, "F", k, hr).start)

    near = far = list(range(half))
    others = range(1, nx)

    def run(local, distant):
        (mk, mo), (tk, to) = local, distant

        def x_out(o):
            for dx in others:
                head_out(dx, 0, target(mk, mo[o])).start()

        for o in reversed(range(half)) if mk == "N" else range(half):
            head_out(0, 0, target(mk, mo[o])).start()
        for o in range(half):
            head_out(0, 1, target(mk, mo[o])).start()
            r = half - 1 - o
            if mk == "F" or r >= early:
                x_out(r)
        for j in range(W_CUTS):
            w_in[j].wait()
            w_out[j].start()
        meet_first()
        if half > 2:
            meet_last()
        for k in reversed(mo) if mk == "N" else mo:
            landed(0, target(mk, k))
            compute(0, mk, k, 0)
        all_w.wait_recv()
        for k in reversed(mo) if mk == "N" else mo:
            compute(0, mk, k, 1)

        def x_land(o):
            for dx in others:
                t = target(mk, mo[o])
                landed(dx, t)
                if o >= early:
                    onward_y(dx, t).start()

        def y_land(o):
            t = target(tk, to[o])
            landed(0, t)
            if o < early:
                for dx in others:
                    onward_x(dx, t).start()

        def diagonal(o):
            for dx in others:
                landed(dx, target(tk, to[o]))
                both(dx, tk, to[o])

        if mk == "N":
            for o in range(half):
                y_land(o)
                if o < early:
                    x_out(early - 1 - o)
                both(0, tk, to[o])
                if half - 1 - o >= early:
                    x_land(half - 1 - o)
        else:
            for o in range(half):
                x_land(half - 1 - o)
                for dx in others:
                    both(dx, mk, mo[half - 1 - o])
                y_land(o)
        if half == 2:
            meet_last()
        if mk == "N":
            for r in reversed(range(early, half)):
                for dx in others:
                    both(dx, mk, mo[r], send=False)
            merge(0, far[0])
            for o in range(half):
                diagonal(o)
            for k in far[1:]:
                merge(0, k)
            for r in reversed(range(early)):
                x_land(r)
                for dx in others:
                    both(dx, mk, mo[r], send=mo[r] == 0)
            for k in far:
                for dx in others:
                    merge(dx, k)
            for k in range(1, half):
                for dx in others:
                    late(dx, k)
        else:
            for k in far:
                merge(0, k)
                both(0, tk, to[half - 1 - k])
            for o in reversed(range(half)):
                diagonal(o)
            for k in reversed(far):
                for dx in others:
                    merge(dx, k)

    pl.when(y == s)(lambda: run(("N", near), ("F", far)))
    pl.when(y != s)(lambda: run(("F", far), ("N", near)))

    gain_in.wait()
    gain_out[...] = gain_v[...].astype(F32).reshape(1, cols)
    res_in.wait()
    total = jnp.zeros((out_rows, 128), F32)
    for dx in range(nx):
        from_x = lax.rem(x - dx + nx, nx)
        for hr in range(CORES):
            side = cross if hr == 0 else core
            where = pl.ds(pl.multiple_of((from_x * CORES + side) * wc, wc), wc)
            if hr == 0:
                group = recv.at[dx, pl.ds(0, half)]
                pltpu.make_async_remote_copy(
                    src_ref=group, dst_ref=group, send_sem=p_send, recv_sem=n_recv.at[dx],
                    device_id=partner, device_id_type=MESH).wait_recv()
            acc = recv[dx, 0, hr].astype(F32)
            for k in range(1, half):
                acc = acc + recv[dx, k, hr].astype(F32)
            to_owner(dx, "F", 0, hr).wait_recv()
            acc = acc + recv[dx, half, hr].astype(F32)
            hidden = (res_v[:, where].astype(F32) + acc).astype(BF16)
            hid_ref[:, where] = hidden
            wide = hidden.astype(F32)
            square = wide * wide
            for k in range(0, wc, 128):
                total = total + square[:, k:k + 128]
    sums[0] = jnp.broadcast_to(jnp.sum(total, axis=1, keepdims=True), (out_rows, 128))
    swap = pltpu.make_async_remote_copy(
        src_ref=sums.at[0], dst_ref=sums.at[1], send_sem=s_send, recv_sem=s_recv,
        device_id=place(0, 1, z), device_id_type=MESH)
    swap.start()

    all_w.wait_send()
    for buf, sem in ((heads, h_send), (send_buf, p_send)):
        pltpu.make_async_remote_copy(
            src_ref=buf, dst_ref=buf, send_sem=sem, recv_sem=w_recv, device_id=partner, device_id_type=MESH).wait_send()
    swap.wait()
    inv_ref[...] = lax.rsqrt((sums[0] + sums[1]) / (cols * ny) + 1e-05)


def finish(hid_ref, inv_ref, gain_ref, out_hid, out_nrm, nrm, sems):
    rows, cols = hid_ref.shape
    cut = rows // FINISH_CUTS
    whole = pltpu.make_async_copy(hid_ref, out_hid, sems.at[FINISH_CUTS])
    whole.start()
    parts = []
    for j in range(FINISH_CUTS):
        at = pl.ds(j * cut, cut)
        nrm[at] = (hid_ref[at].astype(F32) * inv_ref[at, :1] * gain_ref[...]).astype(BF16)
        parts.append(pltpu.make_async_copy(nrm.at[at], out_nrm.at[at], sems.at[j]))
        parts[-1].start()
    for copy in (whole, *parts):
        copy.wait()


def shards(head_out, out_weight, residual, norm_gain):
    ny, ngy, nz = (lax.axis_size(a) for a in ("gx", "gy", "gz"))
    nx = ngy // CORES
    depth, wc = out_weight.shape
    out_rows, cols = residual.shape
    half = nz // 2
    if ny != 2 or nz % 2 or half < 2:
        raise ValueError("unsupported mesh")
    any_spec = pl.BlockSpec(memory_space=pl.ANY)
    vmem = pl.BlockSpec(memory_space=pltpu.VMEM)
    dma, regular = pltpu.SemaphoreType.DMA, pltpu.SemaphoreType.REGULAR
    held = pl.pallas_call(
        functools.partial(project, nx, ny, nz),
        out_shape=[pltpu.VMEM((out_rows, cols), BF16), pltpu.VMEM((out_rows, 128), F32), pltpu.VMEM((1, cols), F32)],
        in_specs=[any_spec] * 4,
        out_specs=[vmem] * 3,
        scratch_shapes=[
            pltpu.VMEM((half, out_rows, depth), BF16),
            pltpu.VMEM((nx * nz, out_rows, depth), BF16),
            pltpu.VMEM((depth, wc), BF16),
            pltpu.VMEM((depth, wc), BF16),
            pltpu.VMEM((out_rows, cols), BF16),
            pltpu.VMEM((cols,), BF16),
            pltpu.VMEM((nx * nz, CORES, out_rows, wc), BF16),
            pltpu.VMEM((nx, half + 1, CORES, out_rows, wc), BF16),
            pltpu.VMEM((nx, half, CORES, out_rows, wc), BF16),
            pltpu.VMEM((nx, half, CORES, out_rows, wc), F32),
            pltpu.VMEM((ny, out_rows, 128), F32),
            dma((3,)), dma((W_CUTS,)), dma, dma, dma, dma((nx, nz)),
            dma, dma((nx,)), dma((nx, CORES)), dma((nx, half, CORES)), dma, dma, regular, regular,
        ],
        compiler_params=pltpu.CompilerParams(collective_id=0, has_side_effects=True),
    )(head_out.reshape(half, out_rows, depth), out_weight, residual, norm_gain)
    return pl.pallas_call(
        finish,
        out_shape=[jax.ShapeDtypeStruct((out_rows, cols), BF16)] * 2,
        in_specs=[vmem] * 3,
        out_specs=[any_spec] * 2,
        scratch_shapes=[pltpu.VMEM((out_rows, cols), BF16), dma((FINISH_CUTS + 1,))],
    )(*(pltpu.with_memory_space_constraint(a, pltpu.VMEM) for a in held))


def solution(mesh):
    in_specs = (P(("gy", "gx"), "gz"), P("gz", ("gx", "gy")), P(("gy", "gz"), "gx"), P())
    out_specs = (P(("gy", "gz"), "gx"), P(("gy", "gz"), "gx"))
    return jax.shard_map(shards, mesh=mesh, in_specs=in_specs, out_specs=out_specs, check_vma=False)
```
